128 devices in a mesh: sector: 64 (over x, y, z_lo, core), dof: 2 (over z_hi).
Axes of the slice: x: 4, y: 4, z: 4 (z_hi: 2, z_lo: 2; z = z_hi * 2 + z_lo), core: 2. Of those that a mesh axis runs over, the one named last changes fastest.
Arguments:
- loads: bfloat16 [64, 128, 32768], P('sector', None, 'dof'), may hold values from -0.75 to 0.75
- modes: bfloat16 [32768, 512], P('dof'), may hold values from -0.25 to 0.25
- response: float32 [64, 128, 512], P('sector', None, 'dof'), may hold values from -6 to 6
- pattern: int32 [64], P('sector'), may hold values from 0 to 7
- deviation: float32 [8, 512], replicated, may hold values from -1 to 1
- eigen: float32 [64, 512], replicated, may hold values from 1 to 10
- loss: float32 [512], replicated, may hold values from 0.2 to 0.6
- omega_sq: float32 [64], replicated, may hold values from 0.5 to 12
- iface_left: int32 [1024], P('dof'), may hold values from 0 to 16383, as said below
- iface_right: int32 [1024], P('dof'), may hold values from 0 to 16383, as said below
Outputs:
- modal_response: float32 [64, 128, 512], P('sector', None, 'dof')
- displacement: bfloat16 [64, 128, 32768], P('sector', None, 'dof')
The draws below stay inside these ranges and needn't reach their ends.
Inputs may be any that keep to these rules, and one draw needn't show every extreme that they name: Within each block of 512 entries, the entries of iface_left and of iface_right together are (2) * 512 distinct rows. `iface_right`: see iface_left.
All inputs are finite; a program needn't handle non-finite values.
Results may differ from the reference program's by a relative error of at most 0.005.
Values may be sent and summed in bfloat16 or wider, within the bound.
No kernel may reach another device: no remote copies, remote signals or barrier semaphores. Data moves between devices by JAX's collectives and lax.ppermute only.
A program may use at most 128 MiB of HBM per device.

```python
import math
import jax
import jax.numpy as jnp
from jax import lax

M = 512
DOF_DEV = 16384
FREQ = 64
IFC_DEV = 512
PATTERNS = 8
SECTORS = 64
DOFS = 32768
IFACE = 1024
N_DOF = 2


def iface_pick(key):
    base = jax.random.fold_in(key, 7)

    def block(number):
        order = jax.random.permutation(jax.random.fold_in(base, number), DOF_DEV)
        return order[:2 * IFC_DEV]
    return jax.vmap(block)(jnp.arange(N_DOF, dtype=jnp.int32))


def draw_iface_left(key, part):
    return iface_pick(key)[:, :IFC_DEV].reshape(-1).astype(jnp.int32)


def draw_iface_right(key, part):
    return iface_pick(key)[:, IFC_DEV:].reshape(-1).astype(jnp.int32)


def set_ends(values, stream_key, least, high):
    extent = values.shape
    index_at = [jax.random.randint(jax.random.fold_in(stream_key, axis), (), 0, extent[axis]) for axis in range(len(extent))]
    values = values.at[tuple(index_at)].set(least)
    longest = extent.index(max(extent))
    index_at[longest] = (index_at[longest] + 1) % extent[longest]
    return values.at[tuple(index_at)].set(high)


def block_levels(rng, extent, split, low, top_value):
    def one(position, blocks):
        heights = jax.random.uniform(jax.random.fold_in(jax.random.fold_in(rng, 6), position), (blocks,), jnp.float32, low / len(split), top_value / len(split))
        return jnp.repeat(jnp.exp(heights), extent[position] // blocks).reshape((-1,) + (1,) * (len(extent) - position - 1))

    gain = one(*split[0])
    for cut in split[1:]:
        gain = gain * one(*cut)
    return gain


def centred(rng, extent, scale, most, split=(), held_as=jnp.bfloat16):
    factor_of = block_levels(rng, extent, split, -0.22, 0.18) if split else 1.0
    result = jax.random.normal(rng, extent, jnp.float32) * scale * factor_of
    return jnp.minimum(jnp.maximum(result, -most), most).astype(held_as)


def setup_inputs(seed: int = 0) -> dict:
    keys = jax.random.split(jax.random.key(seed), 11)
    return {
        "loads": centred(keys[0], (SECTORS, 2 * FREQ, DOFS), (DOFS // M) ** -0.5, 0.75, ((0, 64), (2, 2))),
        "modes": centred(keys[1], (DOFS, M), M ** -0.5, 0.25, ((0, 2),)),
        "response": centred(keys[2], (SECTORS, 2 * FREQ, M), 1.0, 6.0, ((0, 64), (2, 2)), jnp.float32),
        "pattern": set_ends(jax.random.randint(keys[3], (SECTORS,), 0, PATTERNS), jax.random.fold_in(keys[3], 1), 0, PATTERNS - 1).astype(jnp.int32),
        "deviation": jnp.clip(jax.random.uniform(keys[4], (PATTERNS, M), jnp.float32, -1.0, 1.0), -1.0, 1.0),
        "eigen": jnp.clip(jnp.exp(jax.random.uniform(keys[5], (SECTORS, M), jnp.float32, math.log(1.0), math.log(10.0))), 1.0, 10.0),
        "loss": jnp.clip(jnp.exp(jax.random.uniform(keys[6], (M,), jnp.float32, math.log(0.2), math.log(0.6))), 0.2, 0.6),
        "omega_sq": jnp.clip(jax.random.uniform(keys[7], (FREQ,), jnp.float32, 0.5, 12.0), 0.5, 12.0),
        "iface_left": draw_iface_left(jax.random.fold_in(keys[10], 71), 0),
        "iface_right": draw_iface_right(jax.random.fold_in(keys[10], 71), 0),
    }


def reference(loads, modes, response, pattern, deviation, eigen, loss, omega_sq, iface_left, iface_right):
    hp = lax.Precision.HIGHEST
    force = jnp.dot(loads.reshape(SECTORS * 2 * FREQ, DOFS), modes, preferred_element_type=jnp.float32)
    force = force.reshape(SECTORS, 2, FREQ, M)
    dev_rows = deviation[pattern]
    rest = force - dev_rows[:, None, None, :] * response.reshape(SECTORS, 2, FREQ, M)
    index = jnp.arange(SECTORS, dtype=jnp.int32)
    turns = (index[:, None] * index[None, :]) % SECTORS
    theta = turns.astype(jnp.float32) * (2.0 * math.pi / SECTORS)
    cosine = jnp.cos(theta)
    sine = jnp.sin(theta)
    real_part = rest[:, 0].reshape(SECTORS, FREQ * M)
    imag_part = rest[:, 1].reshape(SECTORS, FREQ * M)
    spec_re = jnp.dot(cosine, real_part, precision=hp) + jnp.dot(sine, imag_part, precision=hp)
    spec_im = jnp.dot(cosine, imag_part, precision=hp) - jnp.dot(sine, real_part, precision=hp)
    spec_re = spec_re.reshape(SECTORS, FREQ, M)
    spec_im = spec_im.reshape(SECTORS, FREQ, M)
    shifted = eigen[:, None, :] - omega_sq[None, :, None]
    damped = loss[None, None, :] * eigen[:, None, :]
    denom = shifted * shifted + damped * damped
    solved_re = ((spec_re * shifted + spec_im * damped) / denom).reshape(SECTORS, FREQ * M)
    solved_im = ((spec_im * shifted - spec_re * damped) / denom).reshape(SECTORS, FREQ * M)
    out_re = (jnp.dot(cosine, solved_re, precision=hp) - jnp.dot(sine, solved_im, precision=hp)) / SECTORS
    out_im = (jnp.dot(cosine, solved_im, precision=hp) + jnp.dot(sine, solved_re, precision=hp)) / SECTORS
    modal_response = jnp.stack([out_re, out_im], 1).reshape(SECTORS, 2 * FREQ, M)
    rounded = modal_response.astype(jnp.bfloat16)
    raw = jnp.dot(rounded.reshape(SECTORS * 2 * FREQ, M), modes.T, preferred_element_type=jnp.float32)
    raw = raw.reshape(SECTORS, 2 * FREQ, DOFS).astype(jnp.bfloat16)
    offsets = (jnp.arange(IFACE, dtype=jnp.int32) // IFC_DEV) * DOF_DEV
    left_rows = (iface_left + offsets).astype(jnp.int32)
    right_rows = (iface_right + offsets).astype(jnp.int32)
    left_vals = raw[:, :, left_rows].astype(jnp.float32)
    right_vals = raw[:, :, right_rows].astype(jnp.float32)
    right_new = (0.5 * (right_vals + jnp.roll(left_vals, -1, axis=0))).astype(jnp.bfloat16)
    left_new = (0.5 * (jnp.roll(right_vals, 1, axis=0) + left_vals)).astype(jnp.bfloat16)
    displacement = raw.at[:, :, right_rows].set(right_new).at[:, :, left_rows].set(left_new)
    return modal_response, displacement
```

```python
import functools
import math

import jax
import jax.numpy as jnp
import numpy as np
from jax import lax
from jax.experimental import pallas as pl
from jax.experimental.pallas import tpu as pltpu
from jax.sharding import Mesh
from jax.sharding import PartitionSpec as P

SECTOR = ("sector_0", "sector_1", "sector_2", "sector_3")
EVERY = SECTOR + ("dof",)
BF16 = jnp.bfloat16
F32 = jnp.float32
EMPTY = 3.0e38


def one_hot_rows(target):
    out = np.zeros((len(target), int(max(target)) + 1 if len(target) else 0), np.float32)
    out[np.arange(len(target)), target] = 1.0
    return out


def split_bf16(table):
    high = table.astype(np.float32).astype(jnp.bfloat16)
    low = (table - high.astype(np.float64)).astype(np.float32).astype(jnp.bfloat16)
    return high, low


def constants(sectors, dofs, freqs):
    turns = np.outer(np.arange(sectors), np.arange(sectors)) % sectors
    theta = turns * (2.0 * math.pi / sectors)
    cosine, sine = np.cos(theta), np.sin(theta)
    forward = np.zeros((2, sectors, sectors, dofs, 2))
    for d in range(dofs):
        forward[0, :, :, d, 0] = cosine
        forward[0, :, :, d, 1] = sine
        forward[1, :, :, d, 0] = -sine
        forward[1, :, :, d, 1] = cosine
    forward = forward.reshape(2 * sectors, sectors * dofs * 2)
    inverse = np.zeros((sectors, 2, 2, sectors))
    inverse[:, 0, 0, :] = cosine / sectors
    inverse[:, 0, 1, :] = -sine / sectors
    inverse[:, 1, 0, :] = sine / sectors
    inverse[:, 1, 1, :] = cosine / sectors
    inverse = inverse.reshape(2 * sectors, 2 * sectors)
    return split_bf16(forward), split_bf16(inverse)


def dot(a, b):
    return jnp.dot(a, b, preferred_element_type=F32)


def dot_t(a, b):
    return lax.dot_general(a, b, (((1,), (1,)), ((), ())), preferred_element_type=F32)


def one_hot(rows, cols, target):
    at = lax.broadcasted_iota(jnp.int32, (rows, cols), 1)
    row = lax.broadcasted_iota(jnp.int32, (rows, cols), 0)
    return jnp.where(target(row) == at, 1.0, 0.0).astype(BF16)


def force_kernel(steps, pattern, loads, modes, response, deviation, out, total):
    step = pl.program_id(0)

    @pl.when(step == 0)
    def _():
        total[...] = jnp.zeros_like(total)

    total[...] += dot(loads[...], modes[...])

    @pl.when(step == steps - 1)
    def _():
        half = response.shape[1]
        mine = pl.ds(pl.multiple_of(lax.axis_index("dof") * half, half), half)
        row = deviation[pl.ds(pattern[0], 1), mine]
        total[:, mine] -= row * response[...]
        rows = total.shape[0]
        freqs = rows // 2
        stacked = jnp.concatenate([total[:, :half], total[:, half:]], 0).astype(BF16)

        def source(row):
            return (row // 2 % 2) * rows + (row % 2) * freqs + row // 4

        order = one_hot(2 * rows, 2 * rows, source)
        out[...] = dot(order, stacked).astype(BF16)


def force(loads, modes, response, pattern, deviation):
    rows, depth = loads.shape
    width = modes.shape[1]
    half = response.shape[1]
    block = 2048
    steps = depth // block
    return pl.pallas_call(
        functools.partial(force_kernel, steps),
        grid=(steps,),
        out_shape=jax.ShapeDtypeStruct((2 * rows, half), BF16),
        in_specs=[
            pl.BlockSpec(memory_space=pltpu.SMEM),
            pl.BlockSpec((rows, block), lambda k: (0, k)),
            pl.BlockSpec((block, width), lambda k: (k, 0)),
            pl.BlockSpec((rows, half), lambda k: (0, 0)),
            pl.BlockSpec(deviation.shape, lambda k: (0, 0)),
        ],
        out_specs=pl.BlockSpec((2 * rows, half), lambda k: (0, 0)),
        scratch_shapes=[pltpu.VMEM((rows, width), F32)],
        compiler_params=pltpu.CompilerParams(
            dimension_semantics=("arbitrary",), vmem_limit_bytes=24 << 20
        ),
        cost_estimate=pl.CostEstimate(
            flops=2 * rows * depth * width, bytes_accessed=2 * depth * (rows + width), transcendentals=0
        ),
        name="force",
    )(pattern, loads, modes, response, deviation)


def split_here(value):
    high = value.astype(BF16)
    return high, (value - high.astype(F32)).astype(BF16)


def solve_kernel(omega_sq, got, fwd_hi, fwd_lo, inv_hi, inv_lo, eigen, loss, out):
    sectors = eigen.shape[0]
    half = got.shape[1]
    me = lax.axis_index(EVERY)
    side, freq = me % 2, me // 2
    spec = dot(fwd_hi[...], got[...]) + dot(fwd_lo[...], got[...])
    p, q = spec[:sectors], spec[sectors:]
    mine = pl.ds(pl.multiple_of(side * half, half), half)
    stiff = eigen[:, mine]
    a = stiff - omega_sq[freq]
    b = loss[:, mine] * stiff
    denom = a * a + b * b
    solved = jnp.concatenate([(p * a + q * b) / denom, (q * a - p * b) / denom], 0)
    high, low = split_here(solved)
    result = dot(inv_hi[...], high) + (dot(inv_hi[...], low) + dot(inv_lo[...], high))
    result = result.astype(BF16)

    def source(row):
        sector, place = row // 16, row % 8
        near = (sector + place // 2 + sectors - 1) % sectors
        return jnp.where(place < 6, near * 2 + place % 2, -1)

    order = one_hot(out.shape[0], 2 * sectors, source)
    out[...] = dot(order, result).astype(BF16)


def solve(got, fwd, inv, eigen, loss, omega_sq):
    sectors = eigen.shape[0]
    half = got.shape[1]
    whole = lambda s: pl.BlockSpec(memory_space=pltpu.VMEM)
    args = (got, *fwd, *inv, eigen, loss)
    return pl.pallas_call(
        solve_kernel,
        out_shape=jax.ShapeDtypeStruct((sectors * 16, half), BF16),
        in_specs=[pl.BlockSpec(memory_space=pltpu.SMEM)] + [whole(a) for a in args],
        out_specs=pl.BlockSpec(memory_space=pltpu.VMEM),
        compiler_params=pltpu.CompilerParams(vmem_limit_bytes=24 << 20),
        name="solve",
    )(omega_sq, *args)


def recover_kernel(
    tiles, index, got, near, modes, modal, shown, resp, spread, fresh
):
    step = pl.program_id(0)
    rows, width = resp.shape[1:]
    half = got.shape[1]
    freqs = rows // 2
    tile = modes.shape[0]
    entries = near.shape[0]

    @pl.when(step == 0)
    def _():
        per = 256 // 16

        def source(row):
            side, place, f = row // (6 * per), row // per % 6, row % per
            return f * 16 + side * 8 + place

        order = one_hot(12 * per, 256, source)
        for t in range(freqs // per):
            part = dot(order, got[256 * t : 256 * (t + 1), :]).astype(BF16)
            for side in range(2):
                for place in range(6):
                    at = (side * 6 + place) * per
                    resp[
                        place // 2,
                        (place % 2) * freqs + t * per : (place % 2) * freqs + (t + 1) * per,
                        side * half : (side + 1) * half,
                    ] = part[at : at + per]
        mine = pl.ds(pl.multiple_of(lax.axis_index("dof") * half, half), half)
        modal[...] = resp[1, :, mine].astype(F32)

        count = entries // 2
        left, right = near[:count, :], near[count:, :]
        rounded = lambda a, b: dot_t(a, b).astype(BF16).astype(F32)
        fresh[:count, :] = 0.5 * (rounded(right, resp[0]) + rounded(left, resp[1]))
        fresh[count:, :] = 0.5 * (rounded(right, resp[1]) + rounded(left, resp[2]))

        spread[...] = jnp.full(spread.shape, EMPTY, F32)

        def put(i, carry):
            for j in range(8):
                at = i * 8 + j
                spread[pl.ds(index[at], 1), :] = fresh[pl.ds(at, 1), :]
            return carry

        lax.fori_loop(0, entries // 8, put, 0)

    raw = dot_t(resp[1], modes[...]).astype(BF16)
    here = spread[pl.ds(pl.multiple_of(step * tile, tile), tile), :].astype(BF16).T
    shown[...] = jnp.where(here < 1e38, here, raw)


def recover(got, near, modes, index, rows, half):
    depth, width = modes.shape
    tile = 1024
    tiles = depth // tile
    entries = near.shape[0]
    return pl.pallas_call(
        functools.partial(recover_kernel, tiles),
        grid=(tiles,),
        out_shape=(
            jax.ShapeDtypeStruct((rows, half), F32),
            jax.ShapeDtypeStruct((rows, depth), BF16),
        ),
        in_specs=[
            pl.BlockSpec(memory_space=pltpu.SMEM),
            pl.BlockSpec(got.shape, lambda k: (0, 0)),
            pl.BlockSpec(near.shape, lambda k: (0, 0)),
            pl.BlockSpec((tile, width), lambda k: (k, 0)),
        ],
        out_specs=(
            pl.BlockSpec((rows, half), lambda k: (0, 0)),
            pl.BlockSpec((rows, tile), lambda k: (0, k)),
        ),
        scratch_shapes=[
            pltpu.VMEM((3, rows, width), BF16),
            pltpu.VMEM((depth, rows), F32),
            pltpu.VMEM((entries, rows), F32),
        ],
        compiler_params=pltpu.CompilerParams(
            dimension_semantics=("arbitrary",), vmem_limit_bytes=32 << 20
        ),
        name="recover",
    )(index, got, near, modes)


def exchange(pieces):
    return lax.all_to_all(pieces, EVERY, 0, 0, tiled=True)


def shards(
    loads, modes, response, pattern, deviation, eigen, loss, omega_sq, iface_left, iface_right
):
    rows = loads.shape[1]
    half = response.shape[2]
    devices = lax.axis_size(EVERY)
    sectors = lax.axis_size(SECTOR)
    dofs = lax.axis_size("dof")
    fwd, inv = constants(sectors, dofs, rows // 2)
    sent = force(loads[0], modes, response[0], pattern, deviation)
    got = exchange(sent.reshape(devices, -1, half)).reshape(-1, half)
    back = solve(got, fwd, inv, eigen, loss[None], omega_sq)
    index = jnp.concatenate([iface_left, iface_right])
    near = jnp.take(modes, index, axis=0, mode="clip")
    seen = exchange(back.reshape(devices, -1, half)).reshape(-1, half)
    modal, shown = recover(seen, near, modes, index, rows, half)
    return modal[None], shown[None]


def solution(mesh):
    torus = Mesh(
        mesh.devices.reshape(4, 4, 2, 2, mesh.shape["dof"]),
        ("sector_0", "sector_1", "sector_2", "sector_3", "dof"),
    )
    return jax.shard_map(
        shards,
        mesh=torus,
        in_specs=(
            P(SECTOR, None, "dof"),
            P("dof", None),
            P(SECTOR, None, "dof"),
            P(SECTOR),
            P(),
            P(),
            P(),
            P(),
            P("dof"),
            P("dof"),
        ),
        out_specs=(P(SECTOR, None, "dof"), P(SECTOR, None, "dof")),
        check_vma=False,
    )
```

```python
import functools
import math

import jax
import jax.numpy as jnp
import numpy as np
from jax import lax
from jax.experimental import pallas as pl
from jax.experimental.pallas import tpu as pltpu
from jax.sharding import Mesh
from jax.sharding import PartitionSpec as P

SECTOR = ("sector_0", "sector_1", "sector_2", "sector_3")
EVERY = SECTOR + ("dof",)
BF16 = jnp.bfloat16
F32 = jnp.float32
EMPTY = 3.0e38
NEAR = 3


def split_bf16(table):
    high = table.astype(np.float32).astype(jnp.bfloat16)
    low = (table - high.astype(np.float64)).astype(np.float32).astype(jnp.bfloat16)
    return high, low


def transforms(sectors, dofs):
    turns = np.outer(np.arange(sectors), np.arange(sectors)) % sectors
    theta = turns * (2.0 * math.pi / sectors)
    cosine, sine = np.cos(theta), np.sin(theta)
    forward = np.zeros((2, sectors, sectors, dofs, 2))
    for d in range(dofs):
        forward[0, :, :, d, 0] = cosine
        forward[0, :, :, d, 1] = sine
        forward[1, :, :, d, 0] = -sine
        forward[1, :, :, d, 1] = cosine
    forward = forward.reshape(2 * sectors, sectors * dofs * 2)
    inverse = np.zeros((sectors, 2, 2, sectors))
    inverse[:, 0, 0, :] = cosine / sectors
    inverse[:, 0, 1, :] = -sine / sectors
    inverse[:, 1, 0, :] = sine / sectors
    inverse[:, 1, 1, :] = cosine / sectors
    inverse = inverse.reshape(2 * sectors, 2 * sectors)
    return split_bf16(forward), split_bf16(inverse)


def pick(sources, columns):
    sources = np.asarray(sources).reshape(-1)
    out = np.zeros((sources.size, columns), np.float32)
    out[np.arange(sources.size), sources] = 1.0
    return out.astype(jnp.bfloat16)


def send_order(freqs):
    f, side, part = np.meshgrid(np.arange(freqs), np.arange(2), np.arange(2), indexing="ij")
    return pick((side * 2 + part) * freqs + f, 4 * freqs)


def back_order(sectors, dofs):
    s, _, part, lanes = np.meshgrid(
        np.arange(sectors), np.arange(dofs), np.arange(2), np.arange(2), indexing="ij"
    )
    return pick(lanes * 2 * sectors + s * 2 + part, 4 * sectors)


def seen_order(few):
    side, lanes, part, f = np.meshgrid(
        np.arange(2), np.arange(2), np.arange(2), np.arange(few), indexing="ij"
    )
    return pick(((f * 2 + side) * 2 + part) * 2 + lanes, 8 * few)


def dot(a, b):
    return jnp.dot(a, b, preferred_element_type=F32)


def dot_t(a, b):
    return lax.dot_general(a, b, (((1,), (1,)), ((), ())), preferred_element_type=F32)


def part_of(start, size):
    return pl.ds(pl.multiple_of(start * size, size), size)


def within(array, space):
    return pltpu.with_memory_space_constraint(array, space)


def params(mib):
    return pltpu.CompilerParams(vmem_limit_bytes=mib << 20)


AHEAD = 6
SLOTS = 8
GROUP = 32
ROWS = 8


def gather_rows(index, held, near, first_out):
    row = lax.broadcasted_iota(jnp.int32, (8, 128), 0)
    shape = (GROUP, GROUP * ROWS)
    lane = lax.broadcasted_iota(jnp.int32, shape, 1) - ROWS * lax.broadcasted_iota(
        jnp.int32, shape, 0
    )
    width = held.shape[2]
    for first in range(0, index.shape[0], GROUP):
        blocks, places = [], []
        for j in range(GROUP):
            if j % 8 == 0:
                at = jnp.zeros((8, 128), jnp.int32)
            entry = index[first + j]
            blocks.append(held[lax.shift_right_logical(entry, 3)])
            at = jnp.where(row == j % 8, entry, at)
            if j % 8 == 7:
                places.append(at & (ROWS - 1))
        at = jnp.concatenate(places, 0)
        at = jnp.concatenate([at] * (GROUP * ROWS // 128), 1)
        order = jnp.where(lane == at, 1.0, 0.0).astype(BF16)
        chosen = dot(order, jnp.stack(blocks, 0).reshape(GROUP * ROWS, width)).astype(BF16)
        near[first_out + first : first_out + first + GROUP, :] = chosen


def force_kernel(
    pattern, loads, modes, response, deviation, order, left_in, right_in,
    out, turned, near, spread,
    held, brought, total, acted, table, sorter, left, right,
    load_sems, mode_sems, other_sems
):
    width = modes.shape[2]
    depth = modes.shape[0] * ROWS
    block = depth // mode_sems.shape[0]
    steps = depth // block
    others = [
        pltpu.make_async_copy(response, acted, other_sems.at[0]),
        pltpu.make_async_copy(deviation, table, other_sems.at[1]),
        pltpu.make_async_copy(order, sorter, other_sems.at[2]),
        pltpu.make_async_copy(left_in, left, other_sems.at[3]),
        pltpu.make_async_copy(right_in, right, other_sems.at[4]),
    ]

    def copies(k):
        cut = part_of(k, block)
        blocks = part_of(k, block // ROWS)
        return (
            pltpu.make_async_copy(modes.at[blocks], held.at[blocks], mode_sems.at[k]),
            pltpu.make_async_copy(
                loads.at[:, cut], brought.at[lax.rem(k, SLOTS)], load_sems.at[k]
            ),
        )

    for k in range(AHEAD):
        for c in copies(k):
            c.start()
    for c in others:
        c.start()
    total[...] = jnp.zeros_like(total)
    size = 256

    def step(k, carry):
        for c in copies(k):
            c.wait()

        @pl.when(k + AHEAD < steps)
        def _():
            for c in copies(k + AHEAD):
                c.start()

        blocks = held[part_of(k, block // ROWS)].reshape(block, width)
        total[...] += dot(brought[lax.rem(k, SLOTS)], blocks)
        for j in range(block // size):
            here = part_of(k * (block // size) + j, size)
            turned[:, here] = held[part_of(k * (block // size) + j, size // ROWS)].reshape(size, width).T
            spread[here, :] = jnp.full((size, spread.shape[1]), EMPTY, F32)
        return carry

    lax.fori_loop(0, steps, step, 0)
    for c in others:
        c.wait()
    half = acted.shape[1]
    mine = part_of(lax.axis_index("dof"), half)
    total[:, mine] -= table[pl.ds(pattern[0], 1), mine] * acted[...]
    stacked = jnp.concatenate([total[:, :half], total[:, half:]], 0).astype(BF16)
    out[...] = dot(sorter[...], stacked).astype(BF16).reshape(out.shape)
    gather_rows(left, held, near, 0)
    gather_rows(right, held, near, left.shape[0])


def force(loads, modes, response, pattern, deviation, order, left, right):
    rows, depth = loads.shape
    width = modes.shape[1]
    half = response.shape[1]
    steps = 16
    entries = left.shape[0]
    vmem = pl.BlockSpec(memory_space=pltpu.VMEM)
    hbm = pl.BlockSpec(memory_space=pltpu.HBM)
    args = (loads, modes.reshape(depth // ROWS, ROWS, width), response, deviation, order, left, right)
    args = [within(a, pltpu.HBM) for a in args]
    return pl.pallas_call(
        force_kernel,
        out_shape=(
            pltpu.VMEM((rows, 2, half), BF16),
            pltpu.VMEM((width, depth), BF16),
            pltpu.VMEM((2 * entries, width), BF16),
            pltpu.VMEM((depth, rows), F32),
        ),
        in_specs=[pl.BlockSpec(memory_space=pltpu.SMEM)] + [hbm] * len(args),
        out_specs=(vmem,) * 4,
        scratch_shapes=[
            pltpu.VMEM((depth // ROWS, ROWS, width), BF16),
            pltpu.VMEM((SLOTS, rows, depth // steps), BF16),
            pltpu.VMEM((rows, width), F32),
            pltpu.VMEM((rows, half), F32),
            pltpu.VMEM(deviation.shape, F32),
            pltpu.VMEM(order.shape, BF16),
            pltpu.SMEM((entries,), jnp.int32),
            pltpu.SMEM((entries,), jnp.int32),
            pltpu.SemaphoreType.DMA((steps,)),
            pltpu.SemaphoreType.DMA((steps,)),
            pltpu.SemaphoreType.DMA((6,)),
        ],
        compiler_params=params(21),
        cost_estimate=pl.CostEstimate(
            flops=2 * rows * depth * width, bytes_accessed=2 * depth * (rows + width), transcendentals=0
        ),
        name="force",
    )(pattern, *args)


def split_here(value):
    high = value.astype(BF16)
    return high, (value - high.astype(F32)).astype(BF16)


def solve_kernel(omega_sq, got, fwd_hi, fwd_lo, inv_hi, inv_lo, order, eigen, loss, out):
    sectors = eigen.shape[0]
    half = got.shape[-1]
    me = lax.axis_index(EVERY)
    side, freq = me % 2, me // 2
    rows = got[...].reshape(-1, half)
    spec = dot(fwd_hi[...], rows) + dot(fwd_lo[...], rows)
    p, q = spec[:sectors], spec[sectors:]
    mine = part_of(side, half)
    stiff = eigen[:, mine]
    a = stiff - omega_sq[freq]
    b = loss[:, mine] * stiff
    denom = a * a + b * b
    solved = jnp.concatenate([(p * a + q * b) / denom, (q * a - p * b) / denom], 0)
    high, low = split_here(solved)
    own = dot(inv_hi[...], high) + (dot(inv_hi[...], low) + dot(inv_lo[...], high))
    before = jnp.concatenate([own[-2:], own[:-2]], 0)
    after = jnp.concatenate([own[2:], own[:2]], 0)
    lanes = half // 2
    near = jnp.concatenate(
        [jnp.concatenate([v[:, :lanes], v[:, lanes:]], 0) for v in (before, own, after)], 1
    ).astype(BF16)
    out[...] = dot(order[...], near).astype(BF16).reshape(out.shape)


def solve(got, fwd, inv, order, eigen, loss, omega_sq):
    sectors = eigen.shape[0]
    devices, _, half = got.shape
    vmem = pl.BlockSpec(memory_space=pltpu.VMEM)
    args = (got, *fwd, *inv, order, eigen, loss)
    return pl.pallas_call(
        solve_kernel,
        out_shape=pltpu.VMEM((devices, 4, NEAR * half // 2), BF16),
        in_specs=[pl.BlockSpec(memory_space=pltpu.SMEM)] + [vmem] * len(args),
        out_specs=vmem,
        compiler_params=params(6),
        name="solve",
    )(omega_sq, *args)


PHASES = (6144, 4096, 4096, 2048)


def weave(main, side):
    done = 0
    for i, item in enumerate(main):
        item()
        upto = len(side) * (i + 1) // len(main)
        for other in side[done:upto]:
            other()
        done = upto
    for other in side[done:]:
        other()


def recover_kernel(
    left_in, right_in, got, order, near, turned, spread_in, modal, shown, spread,
    resp, fresh, mine_out, left, right, out_sems, other_sems, *raws
):
    width, depth = turned.shape
    rows = spread.shape[1]
    half = width // 2
    freqs = rows // 2
    entries = left.shape[0]
    lanes = half // 2
    few = order.shape[0] // 8
    indexes = [
        pltpu.make_async_copy(left_in, left, other_sems.at[1]),
        pltpu.make_async_copy(right_in, right, other_sems.at[2]),
    ]
    for c in indexes:
        c.start()
    for t in range(freqs // few):
        part = got[2 * few * t : 2 * few * (t + 1)].reshape(8 * few, NEAR * lanes)
        part = dot(order[...], part).astype(BF16)
        for side in range(2):
            for lane in range(2):
                for p in range(2):
                    at = ((side * 2 + lane) * 2 + p) * few
                    for k in range(NEAR):
                        resp[
                            k * rows + p * freqs + t * few : k * rows + p * freqs + (t + 1) * few,
                            side * half + lane * lanes : side * half + (lane + 1) * lanes,
                        ] = part[at : at + few, k * lanes : (k + 1) * lanes]
    mine = part_of(lax.axis_index("dof"), half)
    mine_out[...] = resp[rows : 2 * rows, mine].astype(F32)
    modal_copy = pltpu.make_async_copy(mine_out, modal, other_sems.at[0])
    modal_copy.start()

    at_right = dot_t(near[entries:, :], resp[: 2 * rows, :]).astype(BF16).astype(F32)
    at_left = dot_t(near[:entries, :], resp[rows:, :]).astype(BF16).astype(F32)
    new = 0.5 * (at_right + at_left)
    fresh[:entries, :] = new[:, :rows]
    fresh[entries:, :] = new[:, rows:]

    for c in indexes:
        c.wait()
    size = 256

    def product(at, buffer, cut):
        def run():
            own = resp[rows : 2 * rows, :]
            buffer[:, cut : cut + size] = dot(own, turned[:, at : at + size]).astype(BF16)

        return run

    def scatter(first, count):
        def run():
            for e in range(first, first + count):
                spread[pl.ds(left[e], 1), :] = fresh[e : e + 1, :]
                spread[pl.ds(right[e], 1), :] = fresh[entries + e : entries + e + 1, :]

        return run

    def select(at, buffer, cut):
        def run():
            here = spread[at : at + size, :].astype(BF16).T
            buffer[:, cut : cut + size] = jnp.where(here < 1e38, here, buffer[:, cut : cut + size])

        return run

    starts = [sum(PHASES[:i]) for i in range(len(PHASES))]
    copies = []

    def finish(i):
        span = PHASES[i]
        part = raws[i]
        copy = pltpu.make_async_copy(
            part, shown.at[:, starts[i] : starts[i] + span], out_sems.at[i]
        )
        copy.start()
        copies.append(copy)

    few = 16
    side = [scatter(first, few) for first in range(0, entries, few)]
    for i, span in enumerate(PHASES):
        main = [product(starts[i] + c, raws[i], c) for c in range(0, span, size)]
        weave(main, side)
        if i:
            finish(i - 1)
        side = [select(starts[i] + c, raws[i], c) for c in range(0, span, size)]
    weave([], side)
    finish(len(PHASES) - 1)
    for c in copies:
        c.wait()
    modal_copy.wait()


def recover(got, order, near, turned, spread, left, right):
    width, depth = turned.shape
    rows = spread.shape[1]
    half = width // 2
    entries = left.shape[0]
    vmem = pl.BlockSpec(memory_space=pltpu.VMEM)
    hbm = pl.BlockSpec(memory_space=pltpu.HBM)
    modal, shown, _ = pl.pallas_call(
        recover_kernel,
        out_shape=(
            pltpu.HBM((rows, half), F32),
            pltpu.HBM((rows, depth), BF16),
            pltpu.VMEM(spread.shape, F32),
        ),
        in_specs=[hbm, hbm] + [vmem] * 5,
        out_specs=(hbm, hbm, vmem),
        input_output_aliases={6: 2},
        scratch_shapes=[
            pltpu.VMEM((NEAR * rows, width), BF16),
            pltpu.VMEM((2 * entries, rows), F32),
            pltpu.VMEM((rows, half), F32),
            pltpu.SMEM((entries,), jnp.int32),
            pltpu.SMEM((entries,), jnp.int32),
            pltpu.SemaphoreType.DMA((len(PHASES),)),
            pltpu.SemaphoreType.DMA((3,)),
            *[pltpu.VMEM((rows, span), BF16) for span in PHASES],
        ],
        compiler_params=params(10),
        name="recover",
    )(
        within(left, pltpu.HBM), within(right, pltpu.HBM), got, order, within(near, pltpu.VMEM), within(turned, pltpu.VMEM),
        within(spread, pltpu.VMEM)
    )
    return modal, shown


def exchange(pieces):
    return lax.all_to_all(pieces, EVERY, 0, 0, tiled=True)


def shards(
    loads, modes, response, pattern, deviation, eigen, loss, omega_sq, iface_left, iface_right
):
    rows = loads.shape[1]
    freqs = rows // 2
    sectors = lax.axis_size(SECTOR)
    dofs = lax.axis_size("dof")
    fwd, inv = transforms(sectors, dofs)
    sent, turned, near, spread = force(
        loads[0], modes, response[0], pattern, deviation, send_order(freqs), iface_left, iface_right
    )
    got = exchange(sent)
    back = solve(got, fwd, inv, back_order(sectors, dofs), eigen, loss[None], omega_sq)
    seen = exchange(back)
    modal, shown = recover(seen, seen_order(32), near, turned, spread, iface_left, iface_right)
    return modal[None], shown[None]


def solution(mesh):
    torus = Mesh(
        mesh.devices.reshape(4, 4, 2, 2, mesh.shape["dof"]),
        ("sector_0", "sector_1", "sector_2", "sector_3", "dof"),
    )
    return jax.shard_map(
        shards,
        mesh=torus,
        in_specs=(
            P(SECTOR, None, "dof"),
            P("dof", None),
            P(SECTOR, None, "dof"),
            P(SECTOR),
            P(),
            P(),
            P(),
            P(),
            P("dof"),
            P("dof"),
        ),
        out_specs=(P(SECTOR, None, "dof"), P(SECTOR, None, "dof")),
        check_vma=False,
    )
```

```python
import functools
import math

import jax
import jax.numpy as jnp
import numpy as np
from jax import lax
from jax.experimental import pallas as pl
from jax.experimental.pallas import tpu as pltpu
from jax.sharding import Mesh
from jax.sharding import PartitionSpec as P

SECTOR = ("sector_0", "sector_1", "sector_2", "sector_3")
EVERY = SECTOR + ("dof",)
BF16 = jnp.bfloat16
F32 = jnp.float32
EMPTY = 3.0e38
NEAR = 3


def split_bf16(table):
    high = table.astype(np.float32).astype(jnp.bfloat16)
    low = (table - high.astype(np.float64)).astype(np.float32).astype(jnp.bfloat16)
    return high, low


def transforms(sectors, dofs):
    turns = np.outer(np.arange(sectors), np.arange(sectors)) % sectors
    theta = turns * (2.0 * math.pi / sectors)
    cosine, sine = np.cos(theta), np.sin(theta)
    forward = np.zeros((2, sectors, sectors, dofs, 2))
    for d in range(dofs):
        forward[0, :, :, d, 0] = cosine
        forward[0, :, :, d, 1] = sine
        forward[1, :, :, d, 0] = -sine
        forward[1, :, :, d, 1] = cosine
    forward = forward.reshape(2 * sectors, sectors * dofs * 2)
    inverse = np.zeros((sectors, 2, 2, sectors))
    inverse[:, 0, 0, :] = cosine / sectors
    inverse[:, 0, 1, :] = -sine / sectors
    inverse[:, 1, 0, :] = sine / sectors
    inverse[:, 1, 1, :] = cosine / sectors
    inverse = inverse.reshape(2 * sectors, 2 * sectors)
    return split_bf16(forward), split_bf16(inverse)


def pick(sources, columns):
    sources = np.asarray(sources).reshape(-1)
    out = np.zeros((sources.size, columns), np.float32)
    out[np.arange(sources.size), sources] = 1.0
    return out.astype(jnp.bfloat16)


def send_order(freqs):
    f, side, part = np.meshgrid(np.arange(freqs), np.arange(2), np.arange(2), indexing="ij")
    return pick((side * 2 + part) * freqs + f, 4 * freqs)


def back_order(sectors, dofs):
    s, _, part, lanes = np.meshgrid(
        np.arange(sectors), np.arange(dofs), np.arange(2), np.arange(2), indexing="ij"
    )
    return pick(lanes * 2 * sectors + s * 2 + part, 4 * sectors)


def seen_order(few):
    side, lanes, part, f = np.meshgrid(
        np.arange(2), np.arange(2), np.arange(2), np.arange(few), indexing="ij"
    )
    return pick(((f * 2 + side) * 2 + part) * 2 + lanes, 8 * few)


def dot(a, b):
    return jnp.dot(a, b, preferred_element_type=F32)


def dot_t(a, b):
    return lax.dot_general(a, b, (((1,), (1,)), ((), ())), preferred_element_type=F32)


def part_of(start, size):
    return pl.ds(pl.multiple_of(start * size, size), size)


def within(array, space):
    return pltpu.with_memory_space_constraint(array, space)


def params(mib):
    return pltpu.CompilerParams(vmem_limit_bytes=mib << 20)


AHEAD = 6
SLOTS = 8
GROUP = 32
ROWS = 8


def gather_rows(index, held, near, first_out):
    row = lax.broadcasted_iota(jnp.int32, (8, 128), 0)
    shape = (GROUP, GROUP * ROWS)
    lane = lax.broadcasted_iota(jnp.int32, shape, 1) - ROWS * lax.broadcasted_iota(
        jnp.int32, shape, 0
    )
    width = held.shape[2]
    for first in range(0, index.shape[0], GROUP):
        blocks, places = [], []
        for j in range(GROUP):
            if j % 8 == 0:
                at = jnp.zeros((8, 128), jnp.int32)
            entry = index[first + j]
            blocks.append(held[lax.shift_right_logical(entry, 3)])
            at = jnp.where(row == j % 8, entry, at)
            if j % 8 == 7:
                places.append(at & (ROWS - 1))
        at = jnp.concatenate(places, 0)
        at = jnp.concatenate([at] * (GROUP * ROWS // 128), 1)
        order = jnp.where(lane == at, 1.0, 0.0).astype(BF16)
        chosen = dot(order, jnp.stack(blocks, 0).reshape(GROUP * ROWS, width)).astype(BF16)
        near[first_out + first : first_out + first + GROUP, :] = chosen


def force_kernel(
    pattern, loads, modes, response, deviation, order, left_in, right_in,
    out, turned, near, spread,
    held, brought, total, acted, table, sorter, left, right,
    load_sems, mode_sems, other_sems
):
    width = modes.shape[2]
    depth = modes.shape[0] * ROWS
    block = depth // mode_sems.shape[0]
    steps = depth // block
    others = [
        pltpu.make_async_copy(response, acted, other_sems.at[0]),
        pltpu.make_async_copy(deviation, table, other_sems.at[1]),
        pltpu.make_async_copy(order, sorter, other_sems.at[2]),
        pltpu.make_async_copy(left_in, left, other_sems.at[3]),
        pltpu.make_async_copy(right_in, right, other_sems.at[4]),
    ]

    def copies(k):
        cut = part_of(k, block)
        blocks = part_of(k, block // ROWS)
        return (
            pltpu.make_async_copy(modes.at[blocks], held.at[blocks], mode_sems.at[k]),
            pltpu.make_async_copy(
                loads.at[:, cut], brought.at[lax.rem(k, SLOTS)], load_sems.at[k]
            ),
        )

    for k in range(AHEAD):
        for c in copies(k):
            c.start()
    for c in others:
        c.start()
    total[...] = jnp.zeros_like(total)
    size = 256

    def step(k, carry):
        for c in copies(k):
            c.wait()

        @pl.when(k + AHEAD < steps)
        def _():
            for c in copies(k + AHEAD):
                c.start()

        blocks = held[part_of(k, block // ROWS)].reshape(block, width)
        total[...] += dot(brought[lax.rem(k, SLOTS)], blocks)
        for j in range(block // size):
            here = part_of(k * (block // size) + j, size)
            turned[:, here] = held[part_of(k * (block // size) + j, size // ROWS)].reshape(size, width).T
            spread[here, :] = jnp.full((size, spread.shape[1]), EMPTY, F32)
        return carry

    lax.fori_loop(0, steps, step, 0)
    for c in others:
        c.wait()
    half = acted.shape[1]
    mine = part_of(lax.axis_index("dof"), half)
    total[:, mine] -= table[pl.ds(pattern[0], 1), mine] * acted[...]
    stacked = jnp.concatenate([total[:, :half], total[:, half:]], 0).astype(BF16)
    out[...] = dot(sorter[...], stacked).astype(BF16).reshape(out.shape)
    gather_rows(left, held, near, 0)
    gather_rows(right, held, near, left.shape[0])


def force(loads, modes, response, pattern, deviation, order, left, right):
    rows, depth = loads.shape
    width = modes.shape[1]
    half = response.shape[1]
    steps = 16
    entries = left.shape[0]
    vmem = pl.BlockSpec(memory_space=pltpu.VMEM)
    hbm = pl.BlockSpec(memory_space=pltpu.HBM)
    args = (loads, modes.reshape(depth // ROWS, ROWS, width), response, deviation, order, left, right)
    args = [within(a, pltpu.HBM) for a in args]
    return pl.pallas_call(
        force_kernel,
        out_shape=(
            pltpu.VMEM((rows, 2, half), BF16),
            pltpu.VMEM((width, depth), BF16),
            pltpu.VMEM((2 * entries, width), BF16),
            pltpu.VMEM((depth, rows), F32),
        ),
        in_specs=[pl.BlockSpec(memory_space=pltpu.SMEM)] + [hbm] * len(args),
        out_specs=(vmem,) * 4,
        scratch_shapes=[
            pltpu.VMEM((depth // ROWS, ROWS, width), BF16),
            pltpu.VMEM((SLOTS, rows, depth // steps), BF16),
            pltpu.VMEM((rows, width), F32),
            pltpu.VMEM((rows, half), F32),
            pltpu.VMEM(deviation.shape, F32),
            pltpu.VMEM(order.shape, BF16),
            pltpu.SMEM((entries,), jnp.int32),
            pltpu.SMEM((entries,), jnp.int32),
            pltpu.SemaphoreType.DMA((steps,)),
            pltpu.SemaphoreType.DMA((steps,)),
            pltpu.SemaphoreType.DMA((6,)),
        ],
        compiler_params=params(21),
        cost_estimate=pl.CostEstimate(
            flops=2 * rows * depth * width, bytes_accessed=2 * depth * (rows + width), transcendentals=0
        ),
        name="force",
    )(pattern, *args)


def split_here(value):
    high = value.astype(BF16)
    return high, (value - high.astype(F32)).astype(BF16)


def solve_kernel(got, fwd_hi, fwd_lo, inv_hi, inv_lo, order, eigen, loss, omega_sq, out):
    sectors = eigen.shape[0]
    half = got.shape[-1]
    me = lax.axis_index(EVERY)
    side, freq = me % 2, me // 2
    rows = got[...].reshape(-1, half)
    spec = dot(fwd_hi[...], rows) + dot(fwd_lo[...], rows)
    p, q = spec[:sectors], spec[sectors:]
    mine = part_of(side, half)
    stiff = eigen[:, mine]
    at = lax.broadcasted_iota(jnp.int32, omega_sq.shape, 1) == freq
    a = stiff - jnp.sum(jnp.where(at, omega_sq[...], 0.0), axis=1, keepdims=True)
    b = loss[:, mine] * stiff
    denom = a * a + b * b
    solved = jnp.concatenate([(p * a + q * b) / denom, (q * a - p * b) / denom], 0)
    high, low = split_here(solved)
    own = dot(inv_hi[...], high) + (dot(inv_hi[...], low) + dot(inv_lo[...], high))
    before = jnp.concatenate([own[-2:], own[:-2]], 0)
    after = jnp.concatenate([own[2:], own[:2]], 0)
    lanes = half // 2
    near = jnp.concatenate(
        [jnp.concatenate([v[:, :lanes], v[:, lanes:]], 0) for v in (before, own, after)], 1
    ).astype(BF16)
    out[...] = dot(order[...], near).astype(BF16).reshape(out.shape)


def solve(got, fwd, inv, order, eigen, loss, omega_sq):
    sectors = eigen.shape[0]
    devices, _, half = got.shape
    vmem = pl.BlockSpec(memory_space=pltpu.VMEM)
    args = (got, *fwd, *inv, order, eigen, loss, omega_sq)
    return pl.pallas_call(
        solve_kernel,
        out_shape=pltpu.VMEM((devices, 4, NEAR * half // 2), BF16),
        in_specs=[vmem] * len(args),
        out_specs=vmem,
        compiler_params=params(6),
        name="solve",
    )(*args)


PHASES = (6144, 4096, 4096, 2048)
PIECE = 1024


def weave(main, side):
    done = 0
    for i, item in enumerate(main):
        item()
        upto = len(side) * (i + 1) // len(main)
        for other in side[done:upto]:
            other()
        done = upto
    for other in side[done:]:
        other()


def recover_kernel(
    left_in, right_in, got, order, near, turned, spread_in, modal, shown, spread,
    resp, fresh, mine_out, left, right, out_sems, other_sems, *raws
):
    width, depth = turned.shape
    rows = spread.shape[1]
    half = width // 2
    freqs = rows // 2
    entries = left.shape[0]
    lanes = half // 2
    few = order.shape[0] // 8
    indexes = [
        pltpu.make_async_copy(left_in, left, other_sems.at[1]),
        pltpu.make_async_copy(right_in, right, other_sems.at[2]),
    ]
    for c in indexes:
        c.start()
    for t in range(freqs // few):
        part = got[2 * few * t : 2 * few * (t + 1)].reshape(8 * few, NEAR * lanes)
        part = dot(order[...], part).astype(BF16)
        for side in range(2):
            for lane in range(2):
                for p in range(2):
                    at = ((side * 2 + lane) * 2 + p) * few
                    for k in range(NEAR):
                        resp[
                            k * rows + p * freqs + t * few : k * rows + p * freqs + (t + 1) * few,
                            side * half + lane * lanes : side * half + (lane + 1) * lanes,
                        ] = part[at : at + few, k * lanes : (k + 1) * lanes]
    mine = part_of(lax.axis_index("dof"), half)
    mine_out[...] = resp[rows : 2 * rows, mine].astype(F32)
    modal_copy = pltpu.make_async_copy(mine_out, modal, other_sems.at[0])
    modal_copy.start()

    at_right = dot_t(near[entries:, :], resp[: 2 * rows, :]).astype(BF16).astype(F32)
    at_left = dot_t(near[:entries, :], resp[rows:, :]).astype(BF16).astype(F32)
    new = 0.5 * (at_right + at_left)
    fresh[:entries, :] = new[:, :rows]
    fresh[entries:, :] = new[:, rows:]

    for c in indexes:
        c.wait()
    size = 256

    def product(at, buffer, cut):
        def run():
            own = resp[rows : 2 * rows, :]
            buffer[:, cut : cut + size] = dot(own, turned[:, at : at + size]).astype(BF16)

        return run

    def scatter(first, count):
        def run():
            for e in range(first, first + count):
                spread[pl.ds(left[e], 1), :] = fresh[e : e + 1, :]
                spread[pl.ds(right[e], 1), :] = fresh[entries + e : entries + e + 1, :]

        return run

    def select(at, buffer, cut):
        def run():
            here = spread[at : at + size, :].astype(BF16).T
            buffer[:, cut : cut + size] = jnp.where(here < 1e38, here, buffer[:, cut : cut + size])

        return run

    starts = [sum(PHASES[:i]) for i in range(len(PHASES))]
    copies = []

    def send(i, cut):
        def run():
            at = starts[i] + cut
            copy = pltpu.make_async_copy(
                raws[i].at[:, cut : cut + PIECE],
                shown.at[:, at : at + PIECE],
                out_sems.at[at // PIECE],
            )
            copy.start()
            copies.append(copy)

        return run

    few = 16
    side = [scatter(first, few) for first in range(0, entries, few)]
    for i, span in enumerate(PHASES):
        main = [product(starts[i] + c, raws[i], c) for c in range(0, span, size)]
        weave(main, side)
        side = []
        for c in range(0, span, size):
            side.append(select(starts[i] + c, raws[i], c))
            if (c + size) % PIECE == 0:
                side.append(send(i, c + size - PIECE))
    weave([], side)
    for c in copies:
        c.wait()
    modal_copy.wait()


def recover(got, order, near, turned, spread, left, right):
    width, depth = turned.shape
    rows = spread.shape[1]
    half = width // 2
    entries = left.shape[0]
    vmem = pl.BlockSpec(memory_space=pltpu.VMEM)
    hbm = pl.BlockSpec(memory_space=pltpu.HBM)
    modal, shown, _ = pl.pallas_call(
        recover_kernel,
        out_shape=(
            pltpu.HBM((rows, half), F32),
            pltpu.HBM((rows, depth), BF16),
            pltpu.VMEM(spread.shape, F32),
        ),
        in_specs=[vmem] * 7,
        out_specs=(hbm, hbm, vmem),
        input_output_aliases={6: 2},
        scratch_shapes=[
            pltpu.VMEM((NEAR * rows, width), BF16),
            pltpu.VMEM((2 * entries, rows), F32),
            pltpu.VMEM((rows, half), F32),
            pltpu.SMEM((entries,), jnp.int32),
            pltpu.SMEM((entries,), jnp.int32),
            pltpu.SemaphoreType.DMA((depth // PIECE,)),
            pltpu.SemaphoreType.DMA((3,)),
            *[pltpu.VMEM((rows, span), BF16) for span in PHASES],
        ],
        compiler_params=params(10),
        name="recover",
    )(
        left, right, got, order, within(near, pltpu.VMEM), within(turned, pltpu.VMEM),
        within(spread, pltpu.VMEM)
    )
    return modal, shown


def exchange(pieces):
    return lax.all_to_all(pieces, EVERY, 0, 0, tiled=True)


def shards(
    loads, modes, response, pattern, deviation, eigen, loss, omega_sq, iface_left, iface_right
):
    rows = loads.shape[1]
    freqs = rows // 2
    sectors = lax.axis_size(SECTOR)
    dofs = lax.axis_size("dof")
    fwd, inv = transforms(sectors, dofs)
    sent, turned, near, spread = force(
        loads[0], modes, response[0], pattern, deviation, send_order(freqs), iface_left, iface_right
    )
    got = exchange(sent)
    back = solve(got, fwd, inv, back_order(sectors, dofs), eigen, loss[None], omega_sq[None])
    seen = exchange(back)
    modal, shown = recover(seen, seen_order(32), near, turned, spread, iface_left, iface_right)
    return modal[None], shown[None]


def solution(mesh):
    torus = Mesh(
        mesh.devices.reshape(4, 4, 2, 2, mesh.shape["dof"]),
        ("sector_0", "sector_1", "sector_2", "sector_3", "dof"),
    )
    return jax.shard_map(
        shards,
        mesh=torus,
        in_specs=(
            P(SECTOR, None, "dof"),
            P("dof", None),
            P(SECTOR, None, "dof"),
            P(SECTOR),
            P(),
            P(),
            P(),
            P(),
            P("dof"),
            P("dof"),
        ),
        out_specs=(P(SECTOR, None, "dof"), P(SECTOR, None, "dof")),
        check_vma=False,
    )
```

```python
import functools
import math

import jax
import jax.numpy as jnp
import numpy as np
from jax import lax
from jax.experimental import pallas as pl
from jax.experimental.pallas import tpu as pltpu
from jax.sharding import Mesh
from jax.sharding import PartitionSpec as P

SECTOR = ("sector_0", "sector_1", "sector_2", "sector_3")
ROUTE = ("sector_3", "dof", "sector_2", "sector_1", "sector_0")
BF16 = jnp.bfloat16
F32 = jnp.float32
EMPTY = 3.0e38
NEAR = 3


def split_bf16(table):
    high = table.astype(np.float32).astype(jnp.bfloat16)
    low = (table - high.astype(np.float64)).astype(np.float32).astype(jnp.bfloat16)
    return high, low


def sector_of_device(sizes):
    places = np.unravel_index(np.arange(math.prod(sizes.values())), [sizes[a] for a in ROUTE])
    places = dict(zip(ROUTE, places))
    return np.ravel_multi_index([places[a] for a in SECTOR], [sizes[a] for a in SECTOR])


def transforms(sectors, holders):
    turns = np.outer(np.arange(sectors), np.arange(sectors)) % sectors
    theta = turns * (2.0 * math.pi / sectors)
    cosine, sine = np.cos(theta), np.sin(theta)
    forward = np.zeros((2, sectors, holders.size, 2))
    forward[0, :, :, 0] = cosine[:, holders]
    forward[0, :, :, 1] = sine[:, holders]
    forward[1, :, :, 0] = -sine[:, holders]
    forward[1, :, :, 1] = cosine[:, holders]
    forward = forward.reshape(2 * sectors, holders.size * 2)
    inverse = np.zeros((sectors, 2, 2, sectors))
    inverse[:, 0, 0, :] = cosine / sectors
    inverse[:, 0, 1, :] = -sine / sectors
    inverse[:, 1, 0, :] = sine / sectors
    inverse[:, 1, 1, :] = cosine / sectors
    inverse = inverse.reshape(2 * sectors, 2 * sectors)
    return split_bf16(forward), split_bf16(inverse)


def pick(sources, columns):
    sources = np.asarray(sources).reshape(-1)
    out = np.zeros((sources.size, columns), np.float32)
    out[np.arange(sources.size), sources] = 1.0
    return out.astype(jnp.bfloat16)


def send_order(freqs):
    f, side, part = np.meshgrid(np.arange(freqs), np.arange(2), np.arange(2), indexing="ij")
    return pick((side * 2 + part) * freqs + f, 4 * freqs)


def back_order(sectors, holders):
    s, part, lanes = np.meshgrid(holders, np.arange(2), np.arange(2), indexing="ij")
    return pick(lanes * 2 * sectors + s * 2 + part, 4 * sectors)


def seen_order(few):
    side, lanes, part, f = np.meshgrid(
        np.arange(2), np.arange(2), np.arange(2), np.arange(few), indexing="ij"
    )
    return pick(((f * 2 + side) * 2 + part) * 2 + lanes, 8 * few)


def dot(a, b):
    return jnp.dot(a, b, preferred_element_type=F32)


def dot_t(a, b):
    return lax.dot_general(a, b, (((1,), (1,)), ((), ())), preferred_element_type=F32)


def part_of(start, size):
    return pl.ds(pl.multiple_of(start * size, size), size)


def within(array, space):
    return pltpu.with_memory_space_constraint(array, space)


def params(mib):
    return pltpu.CompilerParams(vmem_limit_bytes=mib << 20)


AHEAD = 6
SLOTS = 8
GROUP = 32
ROWS = 8


def gather_rows(index, held, near, first_out):
    row = lax.broadcasted_iota(jnp.int32, (8, 128), 0)
    shape = (GROUP, GROUP * ROWS)
    lane = lax.broadcasted_iota(jnp.int32, shape, 1) - ROWS * lax.broadcasted_iota(
        jnp.int32, shape, 0
    )
    width = held.shape[2]
    for first in range(0, index.shape[0], GROUP):
        blocks, places = [], []
        for j in range(GROUP):
            if j % 8 == 0:
                at = jnp.zeros((8, 128), jnp.int32)
            entry = index[first + j]
            blocks.append(held[lax.shift_right_logical(entry, 3)])
            at = jnp.where(row == j % 8, entry, at)
            if j % 8 == 7:
                places.append(at & (ROWS - 1))
        at = jnp.concatenate(places, 0)
        at = jnp.concatenate([at] * (GROUP * ROWS // 128), 1)
        order = jnp.where(lane == at, 1.0, 0.0).astype(BF16)
        chosen = dot(order, jnp.stack(blocks, 0).reshape(GROUP * ROWS, width)).astype(BF16)
        near[first_out + first : first_out + first + GROUP, :] = chosen


def force_kernel(
    pattern, loads, modes, response, deviation, order, left_in, right_in,
    out, turned, near, spread,
    held, brought, total, acted, table, sorter, left, right,
    load_sems, mode_sems, other_sems
):
    width = modes.shape[2]
    depth = modes.shape[0] * ROWS
    block = depth // mode_sems.shape[0]
    steps = depth // block
    others = [
        pltpu.make_async_copy(response, acted, other_sems.at[0]),
        pltpu.make_async_copy(deviation, table, other_sems.at[1]),
        pltpu.make_async_copy(order, sorter, other_sems.at[2]),
        pltpu.make_async_copy(left_in, left, other_sems.at[3]),
        pltpu.make_async_copy(right_in, right, other_sems.at[4]),
    ]

    def copies(k):
        cut = part_of(k, block)
        blocks = part_of(k, block // ROWS)
        return (
            pltpu.make_async_copy(modes.at[blocks], held.at[blocks], mode_sems.at[k]),
            pltpu.make_async_copy(
                loads.at[:, cut], brought.at[lax.rem(k, SLOTS)], load_sems.at[k]
            ),
        )

    for k in range(AHEAD):
        for c in copies(k):
            c.start()
    for c in others:
        c.start()
    total[...] = jnp.zeros_like(total)
    size = 256

    def step(k, carry):
        for c in copies(k):
            c.wait()

        @pl.when(k + AHEAD < steps)
        def _():
            for c in copies(k + AHEAD):
                c.start()

        blocks = held[part_of(k, block // ROWS)].reshape(block, width)
        total[...] += dot(brought[lax.rem(k, SLOTS)], blocks)
        for j in range(block // size):
            here = part_of(k * (block // size) + j, size)
            turned[:, here] = held[part_of(k * (block // size) + j, size // ROWS)].reshape(size, width).T
            spread[here, :] = jnp.full((size, spread.shape[1]), EMPTY, F32)
        return carry

    lax.fori_loop(0, steps, step, 0)
    for c in others:
        c.wait()
    half = acted.shape[1]
    mine = part_of(lax.axis_index("dof"), half)
    total[:, mine] -= table[pl.ds(pattern[0], 1), mine] * acted[...]
    stacked = jnp.concatenate([total[:, :half], total[:, half:]], 0).astype(BF16)
    out[...] = dot(sorter[...], stacked).astype(BF16).reshape(out.shape)
    gather_rows(left, held, near, 0)
    gather_rows(right, held, near, left.shape[0])


def force(loads, modes, response, pattern, deviation, order, left, right):
    rows, depth = loads.shape
    width = modes.shape[1]
    half = response.shape[1]
    steps = 16
    entries = left.shape[0]
    vmem = pl.BlockSpec(memory_space=pltpu.VMEM)
    hbm = pl.BlockSpec(memory_space=pltpu.HBM)
    args = (loads, modes.reshape(depth // ROWS, ROWS, width), response, deviation, order, left, right)
    args = [within(a, pltpu.HBM) for a in args]
    return pl.pallas_call(
        force_kernel,
        out_shape=(
            pltpu.VMEM((rows, 2, half), BF16),
            pltpu.VMEM((width, depth), BF16),
            pltpu.VMEM((2 * entries, width), BF16),
            pltpu.VMEM((depth, rows), F32),
        ),
        in_specs=[pl.BlockSpec(memory_space=pltpu.SMEM)] + [hbm] * len(args),
        out_specs=(vmem,) * 4,
        scratch_shapes=[
            pltpu.VMEM((depth // ROWS, ROWS, width), BF16),
            pltpu.VMEM((SLOTS, rows, depth // steps), BF16),
            pltpu.VMEM((rows, width), F32),
            pltpu.VMEM((rows, half), F32),
            pltpu.VMEM(deviation.shape, F32),
            pltpu.VMEM(order.shape, BF16),
            pltpu.SMEM((entries,), jnp.int32),
            pltpu.SMEM((entries,), jnp.int32),
            pltpu.SemaphoreType.DMA((steps,)),
            pltpu.SemaphoreType.DMA((steps,)),
            pltpu.SemaphoreType.DMA((6,)),
        ],
        compiler_params=params(21),
        cost_estimate=pl.CostEstimate(
            flops=2 * rows * depth * width, bytes_accessed=2 * depth * (rows + width), transcendentals=0
        ),
        name="force",
    )(pattern, *args)


def split_here(value):
    high = value.astype(BF16)
    return high, (value - high.astype(F32)).astype(BF16)


def solve_kernel(got, fwd_hi, fwd_lo, inv_hi, inv_lo, order, eigen, loss, omega_sq, out):
    sectors = eigen.shape[0]
    half = got.shape[-1]
    me = lax.axis_index(ROUTE)
    side, freq = me % 2, me // 2
    rows = got[...].reshape(-1, half)
    spec = dot(fwd_hi[...], rows) + dot(fwd_lo[...], rows)
    p, q = spec[:sectors], spec[sectors:]
    mine = part_of(side, half)
    stiff = eigen[:, mine]
    at = lax.broadcasted_iota(jnp.int32, omega_sq.shape, 1) == freq
    a = stiff - jnp.sum(jnp.where(at, omega_sq[...], 0.0), axis=1, keepdims=True)
    b = loss[:, mine] * stiff
    denom = a * a + b * b
    solved = jnp.concatenate([(p * a + q * b) / denom, (q * a - p * b) / denom], 0)
    high, low = split_here(solved)
    own = dot(inv_hi[...], high) + (dot(inv_hi[...], low) + dot(inv_lo[...], high))
    before = jnp.concatenate([own[-2:], own[:-2]], 0)
    after = jnp.concatenate([own[2:], own[:2]], 0)
    lanes = half // 2
    near = jnp.concatenate(
        [jnp.concatenate([v[:, :lanes], v[:, lanes:]], 0) for v in (before, own, after)], 1
    ).astype(BF16)
    out[...] = dot(order[...], near).astype(BF16).reshape(out.shape)


def solve(got, fwd, inv, order, eigen, loss, omega_sq):
    sectors = eigen.shape[0]
    devices, _, half = got.shape
    vmem = pl.BlockSpec(memory_space=pltpu.VMEM)
    args = (got, *fwd, *inv, order, eigen, loss, omega_sq)
    return pl.pallas_call(
        solve_kernel,
        out_shape=pltpu.VMEM((devices, 4, NEAR * half // 2), BF16),
        in_specs=[vmem] * len(args),
        out_specs=vmem,
        compiler_params=params(6),
        name="solve",
    )(*args)


PHASES = (6144, 4096, 4096, 2048)
PIECE = 1024


def weave(main, side):
    done = 0
    for i, item in enumerate(main):
        item()
        upto = len(side) * (i + 1) // len(main)
        for other in side[done:upto]:
            other()
        done = upto
    for other in side[done:]:
        other()


def recover_kernel(
    left_in, right_in, got, order, near, turned, spread_in, modal, shown, spread,
    resp, fresh, mine_out, left, right, out_sems, other_sems, *raws
):
    width, depth = turned.shape
    rows = spread.shape[1]
    half = width // 2
    freqs = rows // 2
    entries = left.shape[0]
    lanes = half // 2
    few = order.shape[0] // 8
    indexes = [
        pltpu.make_async_copy(left_in, left, other_sems.at[1]),
        pltpu.make_async_copy(right_in, right, other_sems.at[2]),
    ]
    for c in indexes:
        c.start()
    for t in range(freqs // few):
        part = got[2 * few * t : 2 * few * (t + 1)].reshape(8 * few, NEAR * lanes)
        part = dot(order[...], part).astype(BF16)
        for side in range(2):
            for lane in range(2):
                for p in range(2):
                    at = ((side * 2 + lane) * 2 + p) * few
                    for k in range(NEAR):
                        resp[
                            k * rows + p * freqs + t * few : k * rows + p * freqs + (t + 1) * few,
                            side * half + lane * lanes : side * half + (lane + 1) * lanes,
                        ] = part[at : at + few, k * lanes : (k + 1) * lanes]
    mine = part_of(lax.axis_index("dof"), half)
    mine_out[...] = resp[rows : 2 * rows, mine].astype(F32)
    modal_copy = pltpu.make_async_copy(mine_out, modal, other_sems.at[0])
    modal_copy.start()

    at_right = dot_t(near[entries:, :], resp[: 2 * rows, :]).astype(BF16).astype(F32)
    at_left = dot_t(near[:entries, :], resp[rows:, :]).astype(BF16).astype(F32)
    new = 0.5 * (at_right + at_left)
    fresh[:entries, :] = new[:, :rows]
    fresh[entries:, :] = new[:, rows:]

    for c in indexes:
        c.wait()
    size = 256

    def product(at, buffer, cut):
        def run():
            own = resp[rows : 2 * rows, :]
            buffer[:, cut : cut + size] = dot(own, turned[:, at : at + size]).astype(BF16)

        return run

    def scatter(first, count):
        def run():
            for e in range(first, first + count):
                spread[pl.ds(left[e], 1), :] = fresh[e : e + 1, :]
                spread[pl.ds(right[e], 1), :] = fresh[entries + e : entries + e + 1, :]

        return run

    def select(at, buffer, cut):
        def run():
            here = spread[at : at + size, :].astype(BF16).T
            buffer[:, cut : cut + size] = jnp.where(here < 1e38, here, buffer[:, cut : cut + size])

        return run

    starts = [sum(PHASES[:i]) for i in range(len(PHASES))]
    copies = []

    def send(i, cut):
        def run():
            at = starts[i] + cut
            copy = pltpu.make_async_copy(
                raws[i].at[:, cut : cut + PIECE],
                shown.at[:, at : at + PIECE],
                out_sems.at[at // PIECE],
            )
            copy.start()
            copies.append(copy)

        return run

    few = 16
    side = [scatter(first, few) for first in range(0, entries, few)]
    for i, span in enumerate(PHASES):
        main = [product(starts[i] + c, raws[i], c) for c in range(0, span, size)]
        weave(main, side)
        side = []
        for c in range(0, span, size):
            side.append(select(starts[i] + c, raws[i], c))
            if (c + size) % PIECE == 0:
                side.append(send(i, c + size - PIECE))
    weave([], side)
    for c in copies:
        c.wait()
    modal_copy.wait()


def recover(got, order, near, turned, spread, left, right):
    width, depth = turned.shape
    rows = spread.shape[1]
    half = width // 2
    entries = left.shape[0]
    vmem = pl.BlockSpec(memory_space=pltpu.VMEM)
    hbm = pl.BlockSpec(memory_space=pltpu.HBM)
    modal, shown, _ = pl.pallas_call(
        recover_kernel,
        out_shape=(
            pltpu.HBM((rows, half), F32),
            pltpu.HBM((rows, depth), BF16),
            pltpu.VMEM(spread.shape, F32),
        ),
        in_specs=[vmem] * 7,
        out_specs=(hbm, hbm, vmem),
        input_output_aliases={6: 2},
        scratch_shapes=[
            pltpu.VMEM((NEAR * rows, width), BF16),
            pltpu.VMEM((2 * entries, rows), F32),
            pltpu.VMEM((rows, half), F32),
            pltpu.SMEM((entries,), jnp.int32),
            pltpu.SMEM((entries,), jnp.int32),
            pltpu.SemaphoreType.DMA((depth // PIECE,)),
            pltpu.SemaphoreType.DMA((3,)),
            *[pltpu.VMEM((rows, span), BF16) for span in PHASES],
        ],
        compiler_params=params(10),
        name="recover",
    )(
        left, right, got, order, within(near, pltpu.VMEM), within(turned, pltpu.VMEM),
        within(spread, pltpu.VMEM)
    )
    return modal, shown


def exchange(pieces):
    return lax.all_to_all(pieces, ROUTE, 0, 0, tiled=True)


def shards(
    loads, modes, response, pattern, deviation, eigen, loss, omega_sq, iface_left, iface_right
):
    rows = loads.shape[1]
    freqs = rows // 2
    sectors = lax.axis_size(SECTOR)
    holders = sector_of_device({axis: lax.axis_size(axis) for axis in ROUTE})
    fwd, inv = transforms(sectors, holders)
    sent, turned, near, spread = force(
        loads[0], modes, response[0], pattern, deviation, send_order(freqs), iface_left, iface_right
    )
    got = exchange(sent)
    back = solve(got, fwd, inv, back_order(sectors, holders), eigen, loss[None], omega_sq[None])
    seen = exchange(back)
    modal, shown = recover(seen, seen_order(32), near, turned, spread, iface_left, iface_right)
    return modal[None], shown[None]


def solution(mesh):
    torus = Mesh(
        mesh.devices.reshape(4, 4, 2, 2, mesh.shape["dof"]),
        ("sector_0", "sector_1", "sector_2", "sector_3", "dof"),
    )
    return jax.shard_map(
        shards,
        mesh=torus,
        in_specs=(
            P(SECTOR, None, "dof"),
            P("dof", None),
            P(SECTOR, None, "dof"),
            P(SECTOR),
            P(),
            P(),
            P(),
            P(),
            P("dof"),
            P("dof"),
        ),
        out_specs=(P(SECTOR, None, "dof"), P(SECTOR, None, "dof")),
        check_vma=False,
    )
```

```python
import functools
import math

import jax
import jax.numpy as jnp
import numpy as np
from jax import lax
from jax.experimental import pallas as pl
from jax.experimental.pallas import tpu as pltpu
from jax.sharding import Mesh
from jax.sharding import PartitionSpec as P

SECTOR = ("sector_0", "sector_1", "sector_2", "sector_3")
ROUTE = ("sector_3", "dof", "sector_2", "sector_1", "sector_0")
BF16 = jnp.bfloat16
F32 = jnp.float32
EMPTY = 3.0e38
NEAR = 3


def split_bf16(table):
    high = table.astype(np.float32).astype(jnp.bfloat16)
    low = (table - high.astype(np.float64)).astype(np.float32).astype(jnp.bfloat16)
    return high, low


def sector_of_device(sizes):
    places = np.unravel_index(np.arange(math.prod(sizes.values())), [sizes[a] for a in ROUTE])
    places = dict(zip(ROUTE, places))
    return np.ravel_multi_index([places[a] for a in SECTOR], [sizes[a] for a in SECTOR])


def transforms(sectors, holders):
    turns = np.outer(np.arange(sectors), np.arange(sectors)) % sectors
    theta = turns * (2.0 * math.pi / sectors)
    cosine, sine = np.cos(theta), np.sin(theta)
    forward = np.zeros((2, sectors, holders.size, 2))
    forward[0, :, :, 0] = cosine[:, holders]
    forward[0, :, :, 1] = sine[:, holders]
    forward[1, :, :, 0] = -sine[:, holders]
    forward[1, :, :, 1] = cosine[:, holders]
    forward = forward.reshape(2 * sectors, holders.size * 2)
    inverse = np.zeros((sectors, 2, 2, sectors))
    inverse[:, 0, 0, :] = cosine / sectors
    inverse[:, 0, 1, :] = -sine / sectors
    inverse[:, 1, 0, :] = sine / sectors
    inverse[:, 1, 1, :] = cosine / sectors
    inverse = inverse.reshape(2 * sectors, 2 * sectors)
    return split_bf16(forward), split_bf16(inverse)


def pick(sources, columns):
    sources = np.asarray(sources).reshape(-1)
    out = np.zeros((sources.size, columns), np.float32)
    out[np.arange(sources.size), sources] = 1.0
    return out.astype(jnp.bfloat16)


def send_order(freqs):
    f, side, part = np.meshgrid(np.arange(freqs), np.arange(2), np.arange(2), indexing="ij")
    return pick((side * 2 + part) * freqs + f, 4 * freqs)


def back_order(sectors, holders):
    s, part, lanes = np.meshgrid(holders, np.arange(2), np.arange(2), indexing="ij")
    return pick(lanes * 2 * sectors + s * 2 + part, 4 * sectors)


def seen_order(few):
    side, lanes, part, f = np.meshgrid(
        np.arange(2), np.arange(2), np.arange(2), np.arange(few), indexing="ij"
    )
    return pick(((f * 2 + side) * 2 + part) * 2 + lanes, 8 * few)


def dot(a, b):
    return jnp.dot(a, b, preferred_element_type=F32)


def dot_t(a, b):
    return lax.dot_general(a, b, (((1,), (1,)), ((), ())), preferred_element_type=F32)


def part_of(start, size):
    return pl.ds(pl.multiple_of(start * size, size), size)


def within(array, space):
    return pltpu.with_memory_space_constraint(array, space)


def params(mib):
    return pltpu.CompilerParams(vmem_limit_bytes=mib << 20)


AHEAD = 4
SLOTS = 5
BLOCK = 1024
LONG = 2 * BLOCK
GROUP = 32
ROWS = 8


def gather_rows(index, held, near, first_out):
    row = lax.broadcasted_iota(jnp.int32, (8, 128), 0)
    shape = (GROUP, GROUP * ROWS)
    lane = lax.broadcasted_iota(jnp.int32, shape, 1) - ROWS * lax.broadcasted_iota(
        jnp.int32, shape, 0
    )
    width = held.shape[2]
    for first in range(0, index.shape[0], GROUP):
        blocks, places = [], []
        for j in range(GROUP):
            if j % 8 == 0:
                at = jnp.zeros((8, 128), jnp.int32)
            entry = index[first + j]
            blocks.append(held[lax.shift_right_logical(entry, 3)])
            at = jnp.where(row == j % 8, entry, at)
            if j % 8 == 7:
                places.append(at & (ROWS - 1))
        at = jnp.concatenate(places, 0)
        at = jnp.concatenate([at] * (GROUP * ROWS // 128), 1)
        order = jnp.where(lane == at, 1.0, 0.0).astype(BF16)
        chosen = dot(order, jnp.stack(blocks, 0).reshape(GROUP * ROWS, width)).astype(BF16)
        near[first_out + first : first_out + first + GROUP, :] = chosen


def force_kernel(
    pattern, loads, modes, response, deviation, order, left_in, right_in,
    out, turned, near, spread,
    held, brought, total, acted, table, sorter, left, right,
    load_sems, mode_sems, other_sems
):
    width = modes.shape[2]
    depth = modes.shape[0] * ROWS
    longs = depth // LONG - 1
    others = [
        pltpu.make_async_copy(response, acted, other_sems.at[0]),
        pltpu.make_async_copy(deviation, table, other_sems.at[1]),
        pltpu.make_async_copy(order, sorter, other_sems.at[2]),
        pltpu.make_async_copy(left_in, left, other_sems.at[3]),
        pltpu.make_async_copy(right_in, right, other_sems.at[4]),
    ]

    def copies(k, short=False):
        span = BLOCK if short else LONG
        place = (k + longs) if short else k
        first = (longs * 2 + k) if short else k
        slot = lax.rem(place, SLOTS)
        return (
            pltpu.make_async_copy(
                modes.at[part_of(first, span // ROWS)],
                held.at[part_of(first, span // ROWS)],
                mode_sems.at[place],
            ),
            pltpu.make_async_copy(
                loads.at[:, part_of(first, span)],
                brought.at[slot, :, pl.ds(0, span)],
                load_sems.at[place],
            ),
        )

    for k in range(AHEAD):
        for c in copies(k):
            c.start()
    for c in others:
        c.start()
    total[...] = jnp.zeros_like(total)
    size = 256

    def use(block, slot, at):
        blocks = held[part_of(block, BLOCK // ROWS)].reshape(BLOCK, width)
        total[...] += dot(brought[slot, :, at : at + BLOCK], blocks)
        for j in range(BLOCK // size):
            piece = block * (BLOCK // size) + j
            here = part_of(piece, size)
            turned[:, here] = held[part_of(piece, size // ROWS)].reshape(size, width).T
            spread[here, :] = jnp.full((size, spread.shape[1]), EMPTY, F32)

    def step(k, carry):
        for c in copies(k):
            c.wait()

        @pl.when(k + AHEAD < longs)
        def _():
            for c in copies(k + AHEAD):
                c.start()

        for short in range(2):

            @pl.when(k + AHEAD == longs + short)
            def _(short=short):
                for c in copies(short, True):
                    c.start()

        slot = lax.rem(k, SLOTS)
        for i in range(LONG // BLOCK):
            use(k * (LONG // BLOCK) + i, slot, i * BLOCK)
        return carry

    lax.fori_loop(0, longs, step, 0)
    for short in range(2):
        for c in copies(short, True):
            c.wait()
        use(longs * 2 + short, (longs + short) % SLOTS, 0)
    for c in others:
        c.wait()
    half = acted.shape[1]
    mine = part_of(lax.axis_index("dof"), half)
    total[:, mine] -= table[pl.ds(pattern[0], 1), mine] * acted[...]
    stacked = jnp.concatenate([total[:, :half], total[:, half:]], 0).astype(BF16)
    out[...] = dot(sorter[...], stacked).astype(BF16).reshape(out.shape)
    gather_rows(left, held, near, 0)
    gather_rows(right, held, near, left.shape[0])


def force(loads, modes, response, pattern, deviation, order, left, right):
    rows, depth = loads.shape
    width = modes.shape[1]
    half = response.shape[1]
    reads = depth // LONG + 1
    entries = left.shape[0]
    vmem = pl.BlockSpec(memory_space=pltpu.VMEM)
    hbm = pl.BlockSpec(memory_space=pltpu.HBM)
    args = (loads, modes.reshape(depth // ROWS, ROWS, width), response, deviation, order, left, right)
    args = [within(a, pltpu.HBM) for a in args]
    return pl.pallas_call(
        force_kernel,
        out_shape=(
            pltpu.VMEM((rows, 2, half), BF16),
            pltpu.VMEM((width, depth), BF16),
            pltpu.VMEM((2 * entries, width), BF16),
            pltpu.VMEM((depth, rows), F32),
        ),
        in_specs=[pl.BlockSpec(memory_space=pltpu.SMEM)] + [hbm] * len(args),
        out_specs=(vmem,) * 4,
        scratch_shapes=[
            pltpu.VMEM((depth // ROWS, ROWS, width), BF16),
            pltpu.VMEM((SLOTS, rows, LONG), BF16),
            pltpu.VMEM((rows, width), F32),
            pltpu.VMEM((rows, half), F32),
            pltpu.VMEM(deviation.shape, F32),
            pltpu.VMEM(order.shape, BF16),
            pltpu.SMEM((entries,), jnp.int32),
            pltpu.SMEM((entries,), jnp.int32),
            pltpu.SemaphoreType.DMA((reads,)),
            pltpu.SemaphoreType.DMA((reads,)),
            pltpu.SemaphoreType.DMA((6,)),
        ],
        compiler_params=params(21),
        cost_estimate=pl.CostEstimate(
            flops=2 * rows * depth * width, bytes_accessed=2 * depth * (rows + width), transcendentals=0
        ),
        name="force",
    )(pattern, *args)


def split_here(value):
    high = value.astype(BF16)
    return high, (value - high.astype(F32)).astype(BF16)


def solve_kernel(got, fwd_hi, fwd_lo, inv_hi, inv_lo, order, eigen, loss, omega_sq, out):
    sectors = eigen.shape[0]
    half = got.shape[-1]
    me = lax.axis_index(ROUTE)
    side, freq = me % 2, me // 2
    rows = got[...].reshape(-1, half)
    spec = dot(fwd_hi[...], rows) + dot(fwd_lo[...], rows)
    p, q = spec[:sectors], spec[sectors:]
    mine = part_of(side, half)
    stiff = eigen[:, mine]
    at = lax.broadcasted_iota(jnp.int32, omega_sq.shape, 1) == freq
    a = stiff - jnp.sum(jnp.where(at, omega_sq[...], 0.0), axis=1, keepdims=True)
    b = loss[:, mine] * stiff
    denom = a * a + b * b
    solved = jnp.concatenate([(p * a + q * b) / denom, (q * a - p * b) / denom], 0)
    high, low = split_here(solved)
    own = dot(inv_hi[...], high) + (dot(inv_hi[...], low) + dot(inv_lo[...], high))
    before = jnp.concatenate([own[-2:], own[:-2]], 0)
    after = jnp.concatenate([own[2:], own[:2]], 0)
    lanes = half // 2
    near = jnp.concatenate(
        [jnp.concatenate([v[:, :lanes], v[:, lanes:]], 0) for v in (before, own, after)], 1
    ).astype(BF16)
    out[...] = dot(order[...], near).astype(BF16).reshape(out.shape)


def solve(got, fwd, inv, order, eigen, loss, omega_sq):
    sectors = eigen.shape[0]
    devices, _, half = got.shape
    vmem = pl.BlockSpec(memory_space=pltpu.VMEM)
    args = (got, *fwd, *inv, order, eigen, loss, omega_sq)
    return pl.pallas_call(
        solve_kernel,
        out_shape=pltpu.VMEM((devices, 4, NEAR * half // 2), BF16),
        in_specs=[vmem] * len(args),
        out_specs=vmem,
        compiler_params=params(6),
        name="solve",
    )(*args)


PHASES = (5120, 4096, 4096, 2048, 1024)
PIECE = 1024


def weave(main, side):
    done = 0
    for i, item in enumerate(main):
        item()
        upto = len(side) * (i + 1) // len(main)
        for other in side[done:upto]:
            other()
        done = upto
    for other in side[done:]:
        other()


def recover_kernel(
    left_in, right_in, got, order, near, turned, spread_in, modal, shown, spread,
    resp, fresh, mine_out, left, right, out_sems, other_sems, *raws
):
    width, depth = turned.shape
    rows = spread.shape[1]
    half = width // 2
    freqs = rows // 2
    entries = left.shape[0]
    lanes = half // 2
    few = order.shape[0] // 8
    indexes = [
        pltpu.make_async_copy(left_in, left, other_sems.at[1]),
        pltpu.make_async_copy(right_in, right, other_sems.at[2]),
    ]
    for c in indexes:
        c.start()
    for t in range(freqs // few):
        part = got[2 * few * t : 2 * few * (t + 1)].reshape(8 * few, NEAR * lanes)
        part = dot(order[...], part).astype(BF16)
        for side in range(2):
            for lane in range(2):
                for p in range(2):
                    at = ((side * 2 + lane) * 2 + p) * few
                    for k in range(NEAR):
                        resp[
                            k * rows + p * freqs + t * few : k * rows + p * freqs + (t + 1) * few,
                            side * half + lane * lanes : side * half + (lane + 1) * lanes,
                        ] = part[at : at + few, k * lanes : (k + 1) * lanes]
    mine = part_of(lax.axis_index("dof"), half)
    mine_out[...] = resp[rows : 2 * rows, mine].astype(F32)
    modal_copy = pltpu.make_async_copy(mine_out, modal, other_sems.at[0])
    modal_copy.start()

    at_right = dot_t(near[entries:, :], resp[: 2 * rows, :]).astype(BF16).astype(F32)
    at_left = dot_t(near[:entries, :], resp[rows:, :]).astype(BF16).astype(F32)
    new = 0.5 * (at_right + at_left)
    fresh[:entries, :] = new[:, :rows]
    fresh[entries:, :] = new[:, rows:]

    for c in indexes:
        c.wait()
    size = 256

    def product(at, buffer, cut):
        def run():
            own = resp[rows : 2 * rows, :]
            buffer[:, cut : cut + size] = dot(own, turned[:, at : at + size]).astype(BF16)

        return run

    def scatter(first, count):
        def run():
            for e in range(first, first + count):
                spread[pl.ds(left[e], 1), :] = fresh[e : e + 1, :]
                spread[pl.ds(right[e], 1), :] = fresh[entries + e : entries + e + 1, :]

        return run

    def select(at, buffer, cut):
        def run():
            here = spread[at : at + size, :].astype(BF16).T
            buffer[:, cut : cut + size] = jnp.where(here < 1e38, here, buffer[:, cut : cut + size])

        return run

    starts = [sum(PHASES[:i]) for i in range(len(PHASES))]
    copies = []

    def send(i, cut):
        def run():
            at = starts[i] + cut
            copy = pltpu.make_async_copy(
                raws[i].at[:, cut : cut + PIECE],
                shown.at[:, at : at + PIECE],
                out_sems.at[at // PIECE],
            )
            copy.start()
            copies.append(copy)

        return run

    few = 16
    side = [scatter(first, few) for first in range(0, entries, few)]
    for i, span in enumerate(PHASES):
        main = [product(starts[i] + c, raws[i], c) for c in range(0, span, size)]
        weave(main, side)
        side = []
        for c in range(0, span, size):
            side.append(select(starts[i] + c, raws[i], c))
            if (c + size) % PIECE == 0:
                side.append(send(i, c + size - PIECE))
    weave([], side)
    for c in copies:
        c.wait()
    modal_copy.wait()


def recover(got, order, near, turned, spread, left, right):
    width, depth = turned.shape
    rows = spread.shape[1]
    half = width // 2
    entries = left.shape[0]
    vmem = pl.BlockSpec(memory_space=pltpu.VMEM)
    hbm = pl.BlockSpec(memory_space=pltpu.HBM)
    modal, shown, _ = pl.pallas_call(
        recover_kernel,
        out_shape=(
            pltpu.HBM((rows, half), F32),
            pltpu.HBM((rows, depth), BF16),
            pltpu.VMEM(spread.shape, F32),
        ),
        in_specs=[vmem] * 7,
        out_specs=(hbm, hbm, vmem),
        input_output_aliases={6: 2},
        scratch_shapes=[
            pltpu.VMEM((NEAR * rows, width), BF16),
            pltpu.VMEM((2 * entries, rows), F32),
            pltpu.VMEM((rows, half), F32),
            pltpu.SMEM((entries,), jnp.int32),
            pltpu.SMEM((entries,), jnp.int32),
            pltpu.SemaphoreType.DMA((depth // PIECE,)),
            pltpu.SemaphoreType.DMA((3,)),
            *[pltpu.VMEM((rows, span), BF16) for span in PHASES],
        ],
        compiler_params=params(10),
        name="recover",
    )(
        left, right, got, order, within(near, pltpu.VMEM), within(turned, pltpu.VMEM),
        within(spread, pltpu.VMEM)
    )
    return modal, shown


def exchange(pieces):
    return lax.all_to_all(pieces, ROUTE, 0, 0, tiled=True)


def shards(
    loads, modes, response, pattern, deviation, eigen, loss, omega_sq, iface_left, iface_right
):
    rows = loads.shape[1]
    freqs = rows // 2
    sectors = lax.axis_size(SECTOR)
    holders = sector_of_device({axis: lax.axis_size(axis) for axis in ROUTE})
    fwd, inv = transforms(sectors, holders)
    sent, turned, near, spread = force(
        loads[0], modes, response[0], pattern, deviation, send_order(freqs), iface_left, iface_right
    )
    got = exchange(sent)
    back = solve(got, fwd, inv, back_order(sectors, holders), eigen, loss[None], omega_sq[None])
    seen = exchange(back)
    modal, shown = recover(seen, seen_order(32), near, turned, spread, iface_left, iface_right)
    return modal[None], shown[None]


def solution(mesh):
    torus = Mesh(
        mesh.devices.reshape(4, 4, 2, 2, mesh.shape["dof"]),
        ("sector_0", "sector_1", "sector_2", "sector_3", "dof"),
    )
    return jax.shard_map(
        shards,
        mesh=torus,
        in_specs=(
            P(SECTOR, None, "dof"),
            P("dof", None),
            P(SECTOR, None, "dof"),
            P(SECTOR),
            P(),
            P(),
            P(),
            P(),
            P("dof"),
            P("dof"),
        ),
        out_specs=(P(SECTOR, None, "dof"), P(SECTOR, None, "dof")),
        check_vma=False,
    )
```
